256 devices in a mesh: groups: 4 (over y, x), expert: 64 (over z, core).
Axes of the slice: x: 2, y: 2, z: 32, core: 2. Of those that a mesh axis runs over, the one named last changes fastest.
The devices are a block of a 4x8x32 slice.
Arguments:
- tokens: bfloat16 [4096, 6144], P(('groups', 'expert')), parts along dimension 0, may hold values from -6 to 6
- route_ids: int32 [4096, 2], P(('groups', 'expert')), parts along dimension 0, may hold values from 0 to 7, all different within a row; in each aligned block of 16 rows (0 to 15, 16 to 31, ...) at most 6 rows name the same one
- route_logits: float32 [4096, 2], P(('groups', 'expert')), parts along dimension 0, may hold values from -6 to 6
- old_place: int32 [64], replicated, may hold values from 0 to 63, each once
- new_place: int32 [64], replicated, may hold values from 0 to 63, each once
- held_gate: bfloat16 [256, 6144, 128], P(('groups', 'expert')), parts along dimension 0, may hold values from -0.078125 to 0.078125
- held_up: bfloat16 [256, 6144, 128], P(('groups', 'expert')), parts along dimension 0, may hold values from -0.078125 to 0.078125
- held_down: bfloat16 [256, 6144, 128], P(('groups', 'expert')), parts along dimension 0, may hold values from -0.1875 to 0.1875
Outputs:
- moe_output: bfloat16 [4096, 6144], P(('groups', 'expert')), parts along dimension 0
- moved_gate: bfloat16 [256, 6144, 128], P(('groups', 'expert')), parts along dimension 0
- moved_up: bfloat16 [256, 6144, 128], P(('groups', 'expert')), parts along dimension 0
- moved_down: bfloat16 [256, 6144, 128], P(('groups', 'expert')), parts along dimension 0
The draws below stay inside these ranges and needn't reach their ends.
There are 4 independent parts, one for each index of `groups`. The reference program is written for one: setup_inputs(seed, part) draws one part's arguments, and reference() takes and returns one part's arrays. A program takes and returns all parts, laid end to end along the dimension named above; an argument that names none is the same for every part. Nothing has to cross between parts.
Inputs may be any that keep to these rules, and one draw needn't show every extreme that they name: `route_ids`: within the rows of one device (aligned blocks of 16 rows) no expert is named by more than 6 rows, a bound that some block reaches; the two ids of a row differ. `old_place`: each device appears once. `new_place`: each device appears once.
All inputs are finite; a program needn't handle non-finite values.
Results may differ from the reference program's by a relative error of at most 0.0058.
Values may be sent and summed in bfloat16 or wider, within the bound.
No kernel may reach another device: no remote copies, remote signals or barrier semaphores. Data moves between devices by JAX's collectives and lax.ppermute only.
A program may use at most 128 MiB of HBM per device.

```python
import math
import jax
import jax.numpy as jnp
import numpy as np
from jax import lax

D = 6144
F_SLOT = 128
EXPERTS = 8
TOP = 2
TOK_DEV = 16
CAP = 6
BLOCKS = 8
HIDDEN_SIZE = 1024
TOKENS = 1024
N_EXPERT = 64


def levels(stream_key, shape, pieces, low, top_value):
    gain, own = 1.0, jax.random.fold_in(stream_key, 6)
    for axis_at, shards_of in pieces:
        heights = jnp.exp(jax.random.uniform(jax.random.fold_in(own, axis_at), (shards_of,), jnp.float32, low / len(pieces), top_value / len(pieces)))
        gain = gain * jnp.repeat(heights, shape[axis_at] // shards_of).reshape([-1 if axis == axis_at else 1 for axis in range(len(shape))])
    return gain


def routed_block(key, own, number, rows, count, top, limit, slope):
    sequence = jax.random.permutation(key, count)
    heavy_load, usual = load_shares(count, rows * top, limit, slope, True), load_shares(count, rows * top, limit, slope, False)
    places = jnp.arange(count)

    def named(tallies, rotation):
        used = int((tallies > 0).sum())
        fixed = max(1, used // 4)
        shifted = fixed + (places - fixed + rotation * (used - fixed)) % max(1, count - fixed)
        return jnp.zeros((count,), jnp.int32).at[sequence[jnp.where(places < fixed, places, shifted)]].set(jnp.asarray(tallies, jnp.int32))

    tallies = jnp.where(number % 4 == 0, named(heavy_load, number // 4), named(usual, number - number // 4 - 1))
    mixed = jax.random.permutation(jax.random.fold_in(own, 3), count)
    giver, taker = mixed[0:count // 2 * 2:2], mixed[1:count // 2 * 2:2]
    room = jnp.minimum(tallies[giver] - 1, limit - tallies[taker]) // 2
    room = jnp.where((giver == sequence[0]) | (taker == sequence[0]) | (tallies[taker] == 0), 0, jnp.maximum(room, 0))
    shifted = jax.random.randint(jax.random.fold_in(own, 4), (count // 2,), 0, 1 << 20) % (room + 1)
    tallies = tallies.at[giver].add(-shifted).at[taker].add(shifted)
    items = jnp.searchsorted(jnp.cumsum(tallies), jnp.arange(rows * top), side="right").astype(jnp.int32)
    table = items.reshape(top, rows).T
    table = table[jax.random.permutation(jax.random.fold_in(own, 1), rows)]
    rotation = jax.random.randint(jax.random.fold_in(own, 2), (rows, 1), 0, top)
    return jnp.take_along_axis(table, (jnp.arange(top)[None, :] + rotation) % top, axis=1)


def load_shares(count, total, most, skew, full):
    loads = [(1 << 20) // math.isqrt(rank ** skew) + 1 for rank in range(1, count + 1)]
    largest = most if full else min(most, max(-(-total // count), total * loads[0] // sum(loads)))
    least = 1 if total - largest >= count - 1 else 0
    holding, spare = [largest] + [least] * (count - 1), total - largest - least * (count - 1)
    while spare > 0:
        movable = [i for i in range(1, count) if holding[i] < largest] or [i for i in range(1, count) if holding[i] < most]
        mass, left = sum([loads[i] for i in movable]), spare
        for i in movable:
            extra = min(most - holding[i], max(1, left * loads[i] // mass), spare)
            holding[i] = holding[i] + extra
            spare = spare - extra
    return np.array(holding)


def noise(stream_key, extent, spread, bound, pieces=(), kind=jnp.bfloat16):
    drawn = jax.random.normal(stream_key, extent, jnp.float32) * spread
    if len(pieces) > 0:
        drawn = levels(stream_key, extent, pieces, -0.22, 0.18) * drawn
    return jnp.clip(drawn, min=-bound, max=bound).astype(kind)


def setup_inputs(seed: int = 0, part: int = 0) -> dict:
    streams_of = jax.random.split(jax.random.key(seed), 9)
    part_keys = jax.random.split(jax.random.fold_in(streams_of[8], part), 9)
    tokens = noise(part_keys[0], (TOKENS, D), 1.0, 6.0, ((0, 64),))
    route_ids_keys = jax.random.split(jax.random.fold_in(part_keys[1], 1), TOKENS // TOK_DEV)
    route_ids_turns = jax.random.permutation(jax.random.fold_in(part_keys[1], 3), TOKENS // TOK_DEV)
    route_ids = jax.vmap(lambda own, number: routed_block(jax.random.fold_in(part_keys[1], 2), own, number, TOK_DEV, EXPERTS, TOP, CAP, 2))(route_ids_keys, route_ids_turns).reshape((TOKENS, TOP))
    route_logits = noise(part_keys[2], (TOKENS, TOP), 1.5, 6.0, ((0, 64),), jnp.float32)
    old_place = jax.random.permutation(streams_of[3], N_EXPERT).astype(jnp.int32)
    new_place = jax.random.permutation(streams_of[4], N_EXPERT).astype(jnp.int32)
    held_gate = noise(part_keys[5], (N_EXPERT, D, F_SLOT), D ** -0.5, 0.078125, ((0, 64),))
    held_up = noise(part_keys[6], (N_EXPERT, D, F_SLOT), D ** -0.5, 0.078125, ((0, 64),))
    held_down = noise(part_keys[7], (N_EXPERT, D, F_SLOT), HIDDEN_SIZE ** -0.5, 0.1875, ((0, 64),))
    return dict(tokens=tokens, route_ids=route_ids, route_logits=route_logits, old_place=old_place, new_place=new_place, held_gate=held_gate, held_up=held_up, held_down=held_down)


def reference(tokens, route_ids, route_logits, old_place, new_place, held_gate, held_up, held_down):
    device_ids = jnp.arange(N_EXPERT, dtype=jnp.int32)
    slot_new_at = jnp.sum(jnp.where(new_place[:, None] == device_ids[None, :], device_ids[:, None], 0), axis=0).astype(jnp.int32)
    source_of = jnp.take(old_place, slot_new_at).astype(jnp.int32)
    moved_gate = jnp.take(held_gate, source_of, axis=0)
    moved_up = jnp.take(held_up, source_of, axis=0)
    moved_down = jnp.take(held_down, source_of, axis=0)
    first_weight = 1.0 / (1.0 + jnp.exp(route_logits[:, 1] - route_logits[:, 0]))
    second_weight = 1.0 / (1.0 + jnp.exp(route_logits[:, 0] - route_logits[:, 1]))
    weights = jnp.stack([first_weight, second_weight], axis=1).astype(jnp.float32)
    expert_ids = jnp.arange(EXPERTS, dtype=jnp.int32)
    route_hits = route_ids[:, :, None] == expert_ids[None, None, :]
    coefficient = jnp.sum(jnp.where(route_hits, weights[:, :, None], 0.0), axis=1).astype(jnp.float32)
    routed = jnp.any(route_hits, axis=1)

    def listing(column):
        return jnp.nonzero(column, size=N_EXPERT * CAP, fill_value=TOKENS)[0].astype(jnp.int32)

    index_table = jax.vmap(listing)(routed.T)
    padded_tokens = jnp.concatenate([tokens, jnp.zeros((1, D), jnp.bfloat16)], axis=0)
    padded_coeff = jnp.concatenate([coefficient, jnp.zeros((1, EXPERTS), jnp.float32)], axis=0)

    def apply_slot(slot_index, accumulated):
        expert_index = slot_index // BLOCKS
        row_index = jnp.take(index_table, expert_index, axis=0).astype(jnp.int32)
        slot_rows = jnp.take(padded_tokens, row_index, axis=0)
        holder = jnp.take(old_place, slot_index).astype(jnp.int32)
        w_gate = jnp.take(held_gate, holder, axis=0)
        w_up = jnp.take(held_up, holder, axis=0)
        w_down = jnp.take(held_down, holder, axis=0)
        gate_value = jnp.dot(slot_rows, w_gate, preferred_element_type=jnp.float32)
        up_value = jnp.dot(slot_rows, w_up, preferred_element_type=jnp.float32)
        hidden = (jax.nn.silu(gate_value) * up_value).astype(jnp.bfloat16)
        partial_value = jnp.dot(hidden, w_down.T, preferred_element_type=jnp.float32).astype(jnp.bfloat16)
        partial_value = lax.optimization_barrier(partial_value).astype(jnp.float32)
        scaling = jnp.take(padded_coeff, row_index, axis=0)[:, expert_index]
        return accumulated.at[row_index].add(scaling[:, None] * partial_value)

    start = jnp.zeros((TOKENS + 1, D), jnp.float32)
    summed = lax.fori_loop(0, N_EXPERT, apply_slot, start)
    moe_output = summed[:TOKENS].astype(jnp.bfloat16)
    return moe_output, moved_gate, moved_up, moved_down
```

```python
import jax
import jax.numpy as jnp
from jax import lax
from jax.sharding import PartitionSpec as P

EXPERTS = 8
EXTRA = 128


def inverse_of(placement, device_ids):
    return jnp.sum(
        jnp.where(placement[:, None] == device_ids[None, :], device_ids[:, None], 0), axis=0
    )


def exact_parts(v):
    first = lax.reduce_precision(v, 8, 7)
    rest = v - first
    second = lax.reduce_precision(rest, 8, 7)
    return first, second, rest - second


def per_device(
    tokens, route_ids, route_logits, old_place, new_place, held_gate, held_up, held_down
):
    devices = lax.axis_size("expert")
    rows, width = tokens.shape
    device_ids = jnp.arange(devices, dtype=jnp.int32)
    slot_new_at = inverse_of(new_place, device_ids)
    slot_old_at = inverse_of(old_place, device_ids)
    source_of = jnp.take(old_place, slot_new_at)

    moved = []
    for held in (held_gate, held_up, held_down):
        f = held.shape[2]
        bands = held.reshape(devices, held.shape[1] // devices, f)
        spread = lax.all_to_all(bands, "expert", split_axis=0, concat_axis=0, tiled=True)
        ordered = jnp.take(spread, source_of, axis=0)
        back = lax.all_to_all(ordered, "expert", split_axis=0, concat_axis=0, tiled=True)
        moved.append(back.reshape(held.shape))

    w0 = 1.0 / (1.0 + jnp.exp(route_logits[:, 1] - route_logits[:, 0]))
    w1 = 1.0 / (1.0 + jnp.exp(route_logits[:, 0] - route_logits[:, 1]))
    columns = [route_ids[:, 0].astype(jnp.float32), route_ids[:, 1].astype(jnp.float32)]
    columns += list(exact_parts(w0)) + list(exact_parts(w1))
    side = jnp.stack(columns, axis=1).astype(jnp.bfloat16)
    side = jnp.pad(side, ((0, 0), (0, EXTRA - side.shape[1])))
    packed = jnp.concatenate([tokens, side], axis=1)
    gathered = lax.all_gather(packed, "expert", axis=0, tiled=True)
    everyone = gathered[:, :width]
    info = gathered[:, width : width + 8].astype(jnp.float32)

    blocks = devices // EXPERTS
    me = lax.axis_index("expert")
    expert = (jnp.take(slot_old_at, me) // blocks).astype(jnp.float32)
    g0 = info[:, 2] + info[:, 3] + info[:, 4]
    g1 = info[:, 5] + info[:, 6] + info[:, 7]
    share = jnp.where(info[:, 0] == expert, g0, 0.0) + jnp.where(info[:, 1] == expert, g1, 0.0)
    gate_value = jnp.dot(everyone, held_gate[0], preferred_element_type=jnp.float32)
    up_value = jnp.dot(everyone, held_up[0], preferred_element_type=jnp.float32)
    hidden = (jax.nn.silu(gate_value) * up_value).astype(jnp.bfloat16)
    partial = lax.dot_general(
        hidden, held_down[0], (((1,), (1,)), ((), ())), preferred_element_type=jnp.float32
    )
    term = (share[:, None] * partial).astype(jnp.bfloat16)
    combined = lax.psum_scatter(term, "expert", scatter_dimension=0, tiled=True)
    return (combined, *moved)


def solution(mesh):
    split = P(("groups", "expert"))
    return jax.shard_map(
        per_device,
        mesh=mesh,
        in_specs=(split, split, split, P(), P(), split, split, split),
        out_specs=(split, split, split, split),
        check_vma=False,
    )
```

```python
import functools

import jax
import jax.numpy as jnp
from jax import lax
from jax.experimental import pallas as pl
from jax.experimental.pallas import tpu as pltpu
from jax.sharding import PartitionSpec as P

EXPERTS = 8
SIDE = 128
ARRAYS = 3
PER = 3
K = ARRAYS * PER
ROWS = 24
NOWHERE = ROWS
MINE, OTHER = 32, 48
T_MAX = 384
SWEEPS = 32
LANES = 128
LANE, EXPERT, MATE, STAYS, CROSS, RIGHT, CORE = range(7)
VMEM = pl.BlockSpec(memory_space=pltpu.VMEM)
SMEM = pl.BlockSpec(memory_space=pltpu.SMEM)
ANY = pl.BlockSpec(memory_space=pl.ANY)


def split_kernel(chips, old_ref, new_ref, me_ref, target_ref, count_ref, facts_ref):
    devices = 2 * chips
    half = chips // 2
    shape = (chips, LANES)
    me = me_ref[0]
    lane = lax.broadcasted_iota(jnp.int32, shape, 1)
    link = lax.broadcasted_iota(jnp.int32, shape, 0)
    spot = lane & (devices - 1)
    target = jnp.minimum(lane, 0)
    slot, mate, source = me * 0, me * 0, me * 0
    for s in range(devices):
        at, to = old_ref[s], new_ref[s]
        target = jnp.where(spot == (at & 1) * chips + (at >> 1), to, target)
        slot = jnp.where(at == me, s, slot)
        mate = jnp.where(at == (me ^ 1), s, mate)
        source = jnp.where(to == me, at, source)
    target_ref[...] = target[:1]

    chip = lane & (chips - 1)
    goal = target >> 1
    first = lane < devices
    far = jnp.where(first, (goal - chip) & (chips - 1), (chip - goal) & (chips - 1))
    past = jnp.where(first, (link - chip) & (chips - 1), (chip - link) & (chips - 1))
    cross = (past < far).astype(jnp.float32)
    start = jnp.where(far < half, 1.0, jnp.where(far == half, 0.5, 0.0)).astype(jnp.float32)
    start = start + jnp.minimum(link, 0).astype(jnp.float32)

    def over(v):
        return jnp.broadcast_to(v, shape)

    def sweep(i, carry):
        share, best, best_load = carry
        on = cross * share
        load_cw = over(jnp.sum(jnp.where(first, on, 0.0), axis=1, keepdims=True))
        load_cc = over(jnp.sum(jnp.where(first, 0.0, on), axis=1, keepdims=True))
        top = over(jnp.max(jnp.maximum(load_cw, load_cc), axis=0, keepdims=True))
        best = jnp.where(top < best_load, share, best)
        best_load = jnp.minimum(best_load, top)
        heat = jnp.exp(2.0 * (jnp.where(first, load_cw, load_cc) - top))
        cost = over(jnp.sum(cross * heat, axis=0, keepdims=True))
        sums = over(jnp.sum(heat, axis=0, keepdims=True))
        total = sums + pltpu.roll(sums, devices, 1)
        rate = 0.5 / (1.0 + 0.2 * i.astype(jnp.float32))
        step = rate * (cost - pltpu.roll(cost, devices, 1)) / total
        return jnp.clip(share - step, 0.0, 1.0), best, best_load

    big = start + 1e9
    best = lax.fori_loop(0, SWEEPS, sweep, (start, start, big))[1]
    count = jnp.floor(best * K + 0.5).astype(jnp.int32)
    count_ref[...] = count[:1]
    from_lane = (source & 1) * chips + (source >> 1)
    facts_ref[LANE] = (me >> 1) + (me & 1) * chips
    facts_ref[EXPERT] = slot // (devices // EXPERTS)
    facts_ref[MATE] = mate // (devices // EXPERTS)
    facts_ref[STAYS] = jnp.where((source >> 1) == (me >> 1), 1, 0)
    facts_ref[CROSS] = (source ^ me) & 1
    facts_ref[RIGHT] = jnp.max(jnp.where(lane == from_lane, count, 0))
    facts_ref[CORE] = me & 1


def walk_kernel(chips, target_ref, count_ref, facts_ref, moves_ref, steps_ref):
    shape = (ROWS, LANES)
    row = lax.broadcasted_iota(jnp.int32, shape, 0)
    column = lax.broadcasted_iota(jnp.int32, shape, 1)
    flat = lax.broadcasted_iota(jnp.int32, (8, LANES), 0) * LANES + lax.broadcasted_iota(
        jnp.int32, (8, LANES), 1
    )
    core = facts_ref[CORE]
    here_lane = facts_ref[LANE]
    low = column < chips
    count = jnp.broadcast_to(count_ref[...], shape)
    target = jnp.broadcast_to(target_ref[...], shape)
    count_0 = jnp.where(low, count, pltpu.roll(count, chips, 1))
    count_1 = jnp.where(low, pltpu.roll(count, LANES - chips, 1), count)
    target_0 = jnp.where(low, target, pltpu.roll(target, chips, 1))
    target_1 = jnp.where(low, pltpu.roll(target, LANES - chips, 1), target)
    own_0 = row < K
    count = jnp.where(own_0, count_0, count_1)
    target = jnp.where(own_0, target_0, target_1)
    goal = target >> 1
    piece = jnp.where(own_0, row, row - K)
    here = column & (chips - 1)
    far = jnp.where(low, (goal - here) & (chips - 1), (here - goal) & (chips - 1))
    first = jnp.where(low, 0, count)
    final = jnp.where(low, count, K)
    holds = (row < 2 * K) & (far > 0) & (piece >= first) & (piece < final) & (column < 2 * chips)
    code = far * 32 + (target & 1) * K + piece
    state = jnp.where(holds, code * 64 + 63 - row, jnp.where(row < 2 * K, -1, 0))

    def all_rows(v):
        return jnp.broadcast_to(v, shape)

    def step(t, carry):
        state, now, later, last, moves = carry
        came = now - 1
        transit = came >= 32
        free = all_rows(jnp.min(jnp.where(state == 0, row, ROWS - 1), axis=0, keepdims=True))
        state = jnp.where(row == jnp.where(transit, free, -1), came * 64 + 31 - row, state)
        store = jnp.where(transit, free, jnp.where(now > 0, MINE + came, NOWHERE))
        top = all_rows(jnp.max(state, axis=0, keepdims=True))
        some = top > 0
        taken = 31 - (top & 31)
        state = jnp.where(row == jnp.where(some, taken, -1), 0, state)
        load = jnp.where(some, taken + ((top >> 5) & 1) * 64, NOWHERE)
        send = jnp.where(some, (top >> 6) - 31, 0)
        right = jnp.where(
            column == 0, pltpu.roll(send, LANES - chips + 1, 1), pltpu.roll(send, 1, 1)
        )
        left = jnp.where(
            column == 2 * chips - 1, pltpu.roll(send, chips - 1, 1), pltpu.roll(send, LANES - 1, 1)
        )
        both = jnp.where(column == here_lane, store * 128 + load, 0)[:8]
        mine = jnp.broadcast_to(jnp.max(both, axis=1, keepdims=True), (8, LANES))
        moves = jnp.where(flat == t, mine, moves)
        last = jnp.where(now > 0, t, last)
        return state, later, jnp.where(low, right, left), last, moves

    def block(carry):
        t, rest, _ = carry
        for i in range(8):
            rest = step(t + i, rest)
        going = jnp.max(jnp.maximum(rest[0], jnp.maximum(rest[1], rest[2])))
        return t + 8, rest, going

    nothing = jnp.minimum(target, 0)
    moves = jnp.minimum(flat, 0) + NOWHERE * 129
    _, (_, _, _, last, moves), _ = lax.while_loop(
        lambda c: (c[2] > 0) & (c[0] < T_MAX),
        block,
        (jnp.int32(0), (state, nothing, nothing, nothing, moves), jnp.int32(1)),
    )
    steps_ref[0] = jnp.max(last) + 1

    def by_core(d):
        second = jnp.where(d >= K, 1, 0)
        return d - K * second + jnp.where(second == core, MINE, OTHER)

    store, load = moves >> 7, moves & 127
    store = jnp.where(store >= MINE, by_core(store - MINE), store)
    load = jnp.where(load >= 64, by_core(load - 64), load)
    moves_ref[...] = store * 64 + load


def move_kernel(*refs):
    clock, moves, came = refs[:3]
    mine, theirs = refs[3:6], refs[6:9]
    clock_out, send, pool = refs[16:19]
    kept, other = refs[19:22], refs[22:25]
    put, get = refs[25:]
    flat = lax.broadcasted_iota(jnp.int32, (8, LANES), 0) * LANES + lax.broadcasted_iota(
        jnp.int32, (8, LANES), 1
    )
    code = jnp.max(jnp.where(flat == clock[...], moves[...], 0))
    clock_out[...] = clock[...] + 1
    store, load = code >> 6, code & 63
    stores, loads = store != NOWHERE, load != NOWHERE
    straight = (store == load) & (store < NOWHERE)

    def each(place, low, arrays, copy):
        for i, array in enumerate(arrays):
            at = low + PER * i

            @pl.when((place >= at) & (place < at + PER))
            def _(array=array, at=at):
                copy(array.at[place - at]).start()

    def put_to(ref):
        return pltpu.make_async_copy(came.at[0], ref, put)

    def get_from(ref):
        return pltpu.make_async_copy(ref, send.at[0], get)

    @pl.when(straight)
    def _():
        get_from(came.at[0]).start()

    @pl.when(loads & ~straight)
    def _():
        @pl.when(load < MINE)
        def _():
            get_from(pool.at[load]).start()

        @pl.when((load >= MINE) & (load < OTHER))
        def _():
            each(load, MINE, mine, get_from)

        @pl.when(load >= OTHER)
        def _():
            each(load, OTHER, theirs, get_from)

    @pl.when(stores & ~straight)
    def _():
        @pl.when(store < MINE)
        def _():
            put_to(pool.at[store]).start()

        @pl.when((store >= MINE) & (store < OTHER))
        def _():
            each(store, MINE, kept, put_to)

        @pl.when(store >= OTHER)
        def _():
            each(store, OTHER, other, put_to)

        put_to(pool.at[0]).wait()

    @pl.when(loads)
    def _():
        get_from(pool.at[0]).wait()


def new_kernel(*refs):
    pass


def settle_kernel(*refs):
    facts, mine, theirs = refs[0], refs[1:4], refs[4:7]
    kept, buffer, come, go = refs[10:13], *refs[13:]
    chunks = [(i, c) for i in range(ARRAYS) for c in range(PER)]

    for cross, source in ((0, mine), (1, theirs)):

        @pl.when((facts[STAYS] == 1) & (facts[CROSS] == cross))
        def _(source=source):
            ins = [
                pltpu.make_async_copy(source[i].at[c], buffer.at[n], come.at[n])
                for n, (i, c) in enumerate(chunks)
            ]
            outs = [
                pltpu.make_async_copy(buffer.at[n], kept[i].at[c], go.at[n])
                for n, (i, c) in enumerate(chunks)
            ]
            for copy in ins:
                copy.start()
            for copy_in, copy_out in zip(ins, outs):
                copy_in.wait()
                copy_out.start()
            for copy in outs:
                copy.wait()


def finish_kernel(array, facts, got, _, kept, sems):
    chunks = range(array * PER, array * PER + PER)

    def copy(n):
        return pltpu.make_async_copy(got.at[n], kept.at[n], sems.at[n])

    def missing(k):
        right = jnp.where(k < facts[RIGHT], 0, 1)
        return (facts[STAYS] == 0) & (right != facts[CORE])

    for n, k in enumerate(chunks):

        @pl.when(missing(k))
        def _(n=n):
            copy(n).start()

    for n, k in enumerate(chunks):

        @pl.when(missing(k))
        def _(n=n):
            copy(n).wait()


def down_kernel(facts, info_ref, h_mine, h_theirs, w_mine, w_theirs, out):
    info = info_ref[...].astype(jnp.float32)
    first = info[:, 2:3] + info[:, 3:4] + info[:, 4:5]
    second = info[:, 5:6] + info[:, 6:7] + info[:, 7:8]

    def part(expert, h, w):
        expert = expert.astype(jnp.float32)
        share = jnp.where(info[:, 0:1] == expert, first, 0.0)
        share += jnp.where(info[:, 1:2] == expert, second, 0.0)
        product = lax.dot_general(
            h[...], w[...], (((1,), (1,)), ((), ())), preferred_element_type=jnp.float32
        )
        return share * product

    out[...] = part(facts[EXPERT], h_mine, w_mine) + part(facts[MATE], h_theirs, w_theirs)


def down(facts, info, h_mine, h_theirs, w_mine, w_theirs):
    rows, units = h_mine.shape
    width = w_mine.shape[0]
    tile = width // 6
    whole = pl.BlockSpec((rows, units), lambda i: (0, 0))
    band = pl.BlockSpec((tile, units), lambda i: (i, 0))
    return pl.pallas_call(
        down_kernel,
        grid=(width // tile,),
        in_specs=[SMEM, pl.BlockSpec((rows, SIDE), lambda i: (0, 0)), whole, whole, band, band],
        out_specs=pl.BlockSpec((rows, tile), lambda i: (0, i)),
        out_shape=jax.ShapeDtypeStruct((rows, width), jnp.float32),
        cost_estimate=pl.CostEstimate(
            flops=4 * rows * units * width, bytes_accessed=4 * rows * width, transcendentals=0
        ),
        name="down",
    )(facts, info, h_mine, h_theirs, w_mine, w_theirs)


def exact_parts(v):
    first = lax.reduce_precision(v, 8, 7)
    rest = v - first
    second = lax.reduce_precision(rest, 8, 7)
    return first, second, rest - second


def per_device(
    tokens, route_ids, route_logits, old_place, new_place, held_gate, held_up, held_down
):
    devices = lax.axis_size("expert")
    chips = devices // 2
    half = chips // 2
    rows, width = tokens.shape
    tall, units = held_gate.shape[1:]
    chunk = tall // PER
    me = lax.axis_index("expert")
    chip, core = me // 2, me % 2
    bf16, i32 = jnp.bfloat16, jnp.int32
    struct = jax.ShapeDtypeStruct

    def pairs(sign, cores):
        return [
            (2 * c + j, 2 * ((c + (sign if j == 0 else -sign)) % chips) + j)
            for c in range(chips)
            for j in cores
        ]

    def ahead(v, cores=(0, 1)):
        return lax.ppermute(v, "expert", pairs(1, cores))

    def back(v, cores=(0, 1)):
        return lax.ppermute(v, "expert", pairs(-1, cores))

    def swap(v):
        return lax.ppermute(v, "expert", [(i, i ^ 1) for i in range(devices)])

    w0 = 1.0 / (1.0 + jnp.exp(route_logits[:, 1] - route_logits[:, 0]))
    w1 = 1.0 / (1.0 + jnp.exp(route_logits[:, 0] - route_logits[:, 1]))
    columns = [route_ids[:, 0].astype(jnp.float32), route_ids[:, 1].astype(jnp.float32)]
    columns += list(exact_parts(w0)) + list(exact_parts(w1))
    side = jnp.stack(columns, axis=1).astype(bf16)
    side = jnp.pad(side, ((0, 0), (0, SIDE - side.shape[1])))
    packed = jnp.concatenate([tokens, side], axis=1)
    other = swap(packed)
    block = jnp.concatenate(
        [jnp.where(core == 0, packed, other), jnp.where(core == 0, other, packed)], axis=0
    )

    held = [h[0] for h in (held_gate, held_up, held_down)]
    mate = [swap(h) for h in held]
    mine = [h.reshape(PER, chunk, units) for h in held]
    theirs = [h.reshape(PER, chunk, units) for h in mate]

    blocks = []
    block, old_place, new_place = lax.optimization_barrier((block, old_place, new_place))
    target, count, facts = pl.pallas_call(
        functools.partial(split_kernel, chips),
        out_shape=(struct((1, LANES), i32), struct((1, LANES), i32), struct((8,), i32)),
        in_specs=[SMEM, SMEM, SMEM],
        out_specs=(VMEM, VMEM, SMEM),
        name="split",
    )(old_place, new_place, me.reshape(1))
    block = ahead(block)
    blocks.append(block)
    block, target, count = lax.optimization_barrier((block, target, count))
    moves, steps = pl.pallas_call(
        functools.partial(walk_kernel, chips),
        out_shape=(struct((8, LANES), i32), struct((1,), i32)),
        in_specs=[VMEM, VMEM, SMEM],
        out_specs=(VMEM, SMEM),
        name="walk",
    )(target, count, facts)
    block = ahead(block)
    blocks.append(block)

    places = pl.pallas_call(
        new_kernel,
        out_shape=(struct((ROWS, chunk, units), bf16),)
        + (struct((PER, chunk, units), bf16),) * (2 * ARRAYS),
        out_specs=(ANY,) * (1 + 2 * ARRAYS),
        name="places",
    )()

    def near(v):
        return pltpu.with_memory_space_constraint(v, pltpu.VMEM)

    def mover(clock, came, places):
        out = pl.pallas_call(
            move_kernel,
            out_shape=(struct((8, LANES), i32), pltpu.VMEM((1, chunk, units), bf16))
            + tuple(pltpu.HBM(p.shape, p.dtype) for p in places),
            in_specs=[VMEM] * 3 + [ANY] * 13,
            out_specs=(VMEM, VMEM) + (ANY,) * 7,
            input_output_aliases={9 + i: 2 + i for i in range(7)},
            scratch_shapes=[pltpu.SemaphoreType.DMA, pltpu.SemaphoreType.DMA],
            name="move",
        )(clock, moves, near(came), *mine, *theirs, *places)
        return out[0], out[1], tuple(out[2:])

    def advance(carry, others=()):
        clock, send, last, places = carry
        came = ahead(send)
        clock, send, places = mover(clock, last, places)
        send, others = lax.optimization_barrier((send, others))
        return (clock, send, came, places), others

    clock = jnp.zeros((8, LANES), i32)
    nothing = jnp.zeros((1, chunk, units), bf16)
    clock, send, places = mover(clock, nothing, places)
    carry = (clock, send, nothing, places)

    group = 4
    terms = []

    def hidden_of(x, gate, up):
        gate_value = jnp.dot(x, gate, preferred_element_type=jnp.float32)
        up_value = jnp.dot(x, up, preferred_element_type=jnp.float32)
        return (jax.nn.silu(gate_value) * up_value).astype(bf16)

    def hidden(part):
        x = jnp.concatenate(part, axis=0)
        info, x = x[:, width:], x[:, :width]
        return info, hidden_of(x, held[0], held[1]), hidden_of(x, mate[0], mate[1])

    def product(h):
        return down(facts, h[0], h[1], h[2], held[2], mate[2])

    def settle(carry):
        kept = carry[3][1 : 1 + ARRAYS]
        kept = pl.pallas_call(
            settle_kernel,
            out_shape=tuple(struct(p.shape, p.dtype) for p in kept),
            in_specs=[SMEM] + [ANY] * 9,
            out_specs=(ANY,) * 3,
            input_output_aliases={7 + i: i for i in range(3)},
            scratch_shapes=[
                pltpu.VMEM((K, chunk, units), bf16),
                pltpu.SemaphoreType.DMA((K,)),
                pltpu.SemaphoreType.DMA((K,)),
            ],
            name="settle",
        )(facts, *mine, *theirs, *kept)
        return (*carry[:3], (carry[3][0], *kept, *carry[3][1 + ARRAYS :]))

    for r in range(2, half):
        block = ahead(block, (0, 1) if r < half - 1 else (0,))
        job = None
        if r % group == 0:
            job = hidden(blocks[r - group :] + ([] if terms else [packed]))
        elif r % group == 1 and r > group:
            job = product(h)
        elif r == group + 2:
            carry = settle(carry)
        carry, (block, job) = advance(carry, (block, job))
        blocks.append(block)
        if r % group == 0:
            h = job
        elif r % group == 1:
            terms.append(job)
    h = hidden(blocks[-group:])
    carry, h = advance(carry, h)
    terms.append(product(h))

    def term(r):
        return terms[r // group][r % group * 2 * rows : (r % group + 1) * 2 * rows]

    total = None
    for r in range(half):
        part = term(half - 1 - r)
        part = part if total is None else part + total.astype(jnp.float32)
        carry, part = advance(carry, part.astype(bf16))
        total = back(part, (0, 1) if r > 0 else (0,))
    carry, total = advance(carry, total)
    give = swap(lax.dynamic_slice_in_dim(total, (1 - core) * rows, rows, 0))
    carry, give = advance(carry, give)
    keep = lax.dynamic_slice_in_dim(total, core * rows, rows, 0)
    own = terms[0][group * 2 * rows :]
    combined = (own + keep.astype(jnp.float32) + give.astype(jnp.float32)).astype(bf16)
    carry, combined = advance(carry, combined)

    done = half - 2 + 1 + half + 3

    def many(n):
        def body(state):
            t, carry = state
            for _ in range(n):
                carry, _ = advance(carry)
            return t + n, carry

        return body

    need = steps[0] - 2
    state = (jnp.int32(done), carry)
    state = lax.while_loop(lambda s: s[0] + 8 <= need, many(8), state)
    state = lax.while_loop(lambda s: s[0] < need, many(2), state)
    clock, _, last, places = state[1]
    places = mover(clock, last, places)[2]

    kept, other = places[1 : 1 + ARRAYS], places[1 + ARRAYS :]
    moved = []
    for i in range(ARRAYS):
        whole = pl.pallas_call(
            functools.partial(finish_kernel, i),
            out_shape=pltpu.HBM((PER, chunk, units), bf16),
            in_specs=[SMEM, VMEM, ANY],
            out_specs=ANY,
            input_output_aliases={2: 0},
            scratch_shapes=[pltpu.SemaphoreType.DMA((PER,))],
            name="finish",
        )(facts, near(swap(other[i])), kept[i])
        moved.append(whole.reshape(1, tall, units))
    return (combined, *moved)


def solution(mesh):
    split = P(("groups", "expert"))
    return jax.shard_map(
        per_device,
        mesh=mesh,
        in_specs=(split, split, split, P(), P(), split, split, split),
        out_specs=(split, split, split, split),
        check_vma=False,
    )
```
